512 devices in a mesh: groups: 2 (over y), seq: 32 (over z), head: 4 (over x), sub: 2 (over core).
Axes of the slice: x: 4, y: 2, z: 32, core: 2. Of those that a mesh axis runs over, the one named last changes fastest.
The devices are a block of a 4x8x32 slice.
Arguments:
- hidden: bfloat16 [8192, 7168], P(('groups', 'seq')), parts along dimension 0, may hold values from -240 to 240
- segment_ids: int32 [8192], P('groups'), parts along dimension 0, may hold values from 0 to 2, never falling along the last dimension, each value on 1 to 2048 neighbouring positions
- attn_gain: float32 [7168], replicated, may hold values from 0.1 to 1.9
- down_weight: bfloat16 [7168, 2112], P('seq', ('head', 'sub')), may hold values from -0.0625 to 0.0625
- q_gain: float32 [1536], replicated, may hold values from 0.1 to 1.9
- kv_gain: float32 [512], replicated, may hold values from 0.1 to 1.9
- q_up: bfloat16 [1536, 12288], P('seq', ('head', 'sub')), may hold values from -0.15625 to 0.15625
- key_up: bfloat16 [8192, 512], P(('head', 'sub'), 'seq'), may hold values from -8 to 8
- value_up: bfloat16 [512, 8192], P('seq', ('head', 'sub')), may hold values from -1 to 1
Outputs:
- attended: bfloat16 [8192, 8192], P(('groups', 'seq'), ('head', 'sub')), parts along dimension 0
The draws below stay inside these ranges and needn't reach their ends.
There are 2 independent parts, one for each index of `groups`. The reference program is written for one: setup_inputs(seed, part) draws one part's arguments, and reference() takes and returns one part's arrays. A program takes and returns all parts, laid end to end along the dimension named above; an argument that names none is the same for every part. Nothing has to cross between parts.
Inputs may be any that keep to these rules, and one draw needn't show every extreme that they name: `segment_ids`: document numbers never fall along the pack.
All inputs are finite; a program needn't handle non-finite values.
Results may differ from the reference program's by a relative error of at most 0.014.
The reference program's roundings to bfloat16 on the way count: a program that leaves them out, or rounds other values in their place, can miss the bound.
Values may be sent and summed in bfloat16 or wider, within the bound.
A program may use at most 64 MiB of HBM per device.

```python
import math
import jax
import jax.numpy as jnp
import numpy as np
from jax import lax

D = 7168
QL = 1536
KVL = 512
ROPE = 64
NOPE = 128
VDIM = 128
H = 64
SEQ_LEN = 4096


def draw_hidden(key, part):
    subkeys = jax.random.split(key, 3)
    row_scale = jnp.exp(jax.random.uniform(subkeys[0], (SEQ_LEN, 1), jnp.float32, 0.0, math.log(10.0)))
    column_ramp = jnp.exp(math.log(3.0) * jnp.arange(D, dtype=jnp.float32) / (D - 1))
    column_scale = column_ramp * jnp.exp(jax.random.uniform(subkeys[1], (D,), jnp.float32, 0.0, math.log(2.0)))
    values = jnp.clip(jax.random.normal(subkeys[2], (SEQ_LEN, D), jnp.float32), -4.0, 4.0)
    return (values * row_scale * column_scale[None, :]).astype(jnp.bfloat16)


def draw_key_up(key, part):
    subkeys = jax.random.split(key, 1)
    base = 2.5 * jnp.clip(jax.random.normal(subkeys[0], (H * NOPE, KVL), jnp.float32), -6.0, 6.0) / math.sqrt(NOPE)
    return base.astype(jnp.bfloat16)


def shard_levels(stream_key, extent, shards, low, high):
    def one(dim, parts):
        steps = jax.random.uniform(jax.random.fold_in(jax.random.fold_in(stream_key, 6), dim), (parts,), jnp.float32, low / len(shards), high / len(shards))
        return jnp.repeat(jnp.exp(steps), extent[dim] // parts).reshape((-1,) + (1,) * (len(extent) - dim - 1))

    level = one(*shards[0])
    for cut in shards[1:]:
        level = level * one(*cut)
    return level


def profile(count, total, most, lean):
    loads = [(1 << 20) // math.isqrt(grade ** lean) + 1 for grade in range(2, count + 1)]
    spare, holding = total - most - (count - 1), [1] * (count - 1)
    while spare > 0:
        movable = [i for i in range(count - 1) if holding[i] < most]
        whole, left = sum([loads[i] for i in movable]), spare
        for i in movable:
            addition = min(most - holding[i], max(1, left * loads[i] // whole), spare)
            holding[i] = holding[i] + addition
            spare = spare - addition
    return np.array([most] + holding)


def uneven(own_key, amount, total, most, skew):
    if amount == 2:
        one = jax.random.randint(own_key, (), max(1, total - most), min(most, total - 1) + 1)
        return jnp.stack([one, total - one])
    sizes = jnp.asarray(profile(amount, total, most, skew), jnp.int32)
    pairs = (amount - 1) // 2
    source_of, taker = sizes[1:1 + 2 * pairs:2], sizes[2:2 + 2 * pairs:2]
    room = jnp.minimum(source_of - 1, most - taker)
    passed = jax.random.randint(jax.random.fold_in(own_key, 1), (pairs,), 0, 1 << 20) % (room + 1)
    sizes = sizes.at[1:1 + 2 * pairs:2].set(source_of - passed).at[2:2 + 2 * pairs:2].set(taker + passed)
    return sizes[jax.random.permutation(jax.random.fold_in(own_key, 2), amount)]


def normal_values(rng, shape, width, limit, cuts=(), kind=jnp.bfloat16):
    loudness = shard_levels(rng, shape, cuts, -0.22, 0.18) if cuts else 1.0
    drawn = jax.random.normal(rng, shape, jnp.float32) * width * loudness
    return jnp.minimum(jnp.maximum(drawn, -limit), limit).astype(kind)


def setup_inputs(seed: int = 0, part: int = 0) -> dict:
    arg_keys = jax.random.split(jax.random.key(seed), 10)
    part_keys = jax.random.split(jax.random.fold_in(arg_keys[9], part), 10)
    hidden = draw_hidden(jax.random.fold_in(jax.random.fold_in(arg_keys[9], part), 71), part)
    segment_ids = jnp.searchsorted(jnp.cumsum(uneven(part_keys[1], 3, SEQ_LEN, SEQ_LEN // 2, 2)), jnp.arange(SEQ_LEN), side="right").astype(jnp.int32)
    attn_gain = jnp.clip(1.0 + 0.18 * jax.random.normal(arg_keys[2], (D,), jnp.float32), 0.1, 1.9)
    down_weight = normal_values(arg_keys[3], (D, QL + KVL + ROPE), D ** -0.5, 0.0625, ((0, 32), (1, 8)))
    q_gain = jnp.clip(1.0 + 0.18 * jax.random.normal(arg_keys[4], (QL,), jnp.float32), 0.1, 1.9)
    kv_gain = jnp.clip(1.0 + 0.18 * jax.random.normal(arg_keys[5], (KVL,), jnp.float32), 0.1, 1.9)
    q_up = normal_values(arg_keys[6], (QL, H * (NOPE + ROPE)), QL ** -0.5, 0.15625, ((0, 32), (1, 8)))
    key_up = draw_key_up(jax.random.fold_in(arg_keys[9], 71), part)
    value_up = normal_values(arg_keys[8], (KVL, H * VDIM), (KVL // 16) ** -0.5, 1.0, ((0, 32), (1, 8)))
    return {"hidden": hidden, "segment_ids": segment_ids, "attn_gain": attn_gain, "down_weight": down_weight, "q_gain": q_gain, "kv_gain": kv_gain, "q_up": q_up, "key_up": key_up, "value_up": value_up}


EPSILON = 1e-06
ROPE_BASE = 10000.0

def rotate(values, positions):
    half_width = values.shape[-1] // 2
    frequency = ROPE_BASE ** (-jnp.arange(half_width, dtype=jnp.float32) / half_width)
    angles = positions.astype(jnp.float32)[:, None] * frequency[None, :]
    target_shape = (angles.shape[0],) + (1,) * (values.ndim - 2) + (half_width,)
    cosine = jnp.cos(angles).reshape(target_shape)
    sine_part = jnp.sin(angles).reshape(target_shape)
    leading = values[..., :half_width]
    second = values[..., half_width:]
    return jnp.concatenate([leading * cosine - second * sine_part, leading * sine_part + second * cosine], axis=-1)

def rms_scale(values):
    return lax.rsqrt(lax.optimization_barrier(jnp.mean(values * values, axis=-1, keepdims=True)) + EPSILON)

def make_keys(columns, positions, kv_gain):
    latent_raw = columns[:, :KVL].astype(jnp.float32)
    latent = (latent_raw * rms_scale(latent_raw) * kv_gain[None, :]).astype(jnp.bfloat16)
    key_rope = rotate(columns[:, KVL:].astype(jnp.float32), positions).astype(jnp.bfloat16)
    return jnp.concatenate([latent, key_rope], axis=1)

def reference(hidden, segment_ids, attn_gain, down_weight, q_gain, kv_gain, q_up, key_up, value_up):
    positions = jnp.arange(SEQ_LEN, dtype=jnp.int32)
    widened = hidden.astype(jnp.float32)
    scaled = (widened * attn_gain[None, :]).astype(jnp.bfloat16)
    down_sum = jnp.dot(scaled, down_weight, preferred_element_type=jnp.float32) * rms_scale(widened)
    down_sum = down_sum.astype(jnp.bfloat16)
    query_low = down_sum[:, :QL].astype(jnp.float32)
    query_latent = (query_low * rms_scale(query_low) * q_gain[None, :]).astype(jnp.bfloat16)
    key_rows = make_keys(down_sum[:, QL:], positions, kv_gain)
    query_full = jnp.dot(query_latent, q_up, preferred_element_type=jnp.float32).astype(jnp.bfloat16)
    query_full = query_full.reshape(SEQ_LEN, H, NOPE + ROPE)
    query_rope = rotate(query_full[:, :, NOPE:].astype(jnp.float32), positions).astype(jnp.bfloat16)
    absorbed = jnp.einsum('shc,hcl->shl', query_full[:, :, :NOPE].astype(jnp.float32), key_up.reshape(H, NOPE, KVL).astype(jnp.float32)).astype(jnp.bfloat16)
    queries = jnp.concatenate([absorbed, query_rope], axis=2)
    allowed = (positions[None, :] <= positions[:, None]) & (segment_ids[None, :] == segment_ids[:, None])
    keys_wide = key_rows.astype(jnp.float32)
    values_wide = key_rows[:, :KVL].astype(jnp.float32)
    score_scale = (NOPE + ROPE) ** (-0.5)

    def one_head(head_queries):
        scores = jnp.dot(head_queries.astype(jnp.float32), keys_wide.T) * score_scale
        scores = jnp.where(allowed, scores, -jnp.inf)
        row_max = lax.optimization_barrier(jnp.max(scores, axis=1, keepdims=True))
        weights = jnp.exp(scores - row_max)
        row_sum = lax.optimization_barrier(jnp.sum(weights, axis=1, keepdims=True))
        rounded = weights.astype(jnp.bfloat16).astype(jnp.float32)
        return (jnp.dot(rounded, values_wide) / row_sum).astype(jnp.bfloat16)
    attended = lax.map(one_head, jnp.transpose(queries, (1, 0, 2)))
    projected = jnp.einsum('hsl,lhv->shv', attended.astype(jnp.float32), value_up.reshape(KVL, H, VDIM).astype(jnp.float32))
    return projected.reshape(SEQ_LEN, H * VDIM).astype(jnp.bfloat16)
```

```python
import functools
import math

import jax
import jax.numpy as jnp
from jax import lax
from jax.experimental import pallas as pl
from jax.experimental.pallas import tpu as pltpu
from jax.sharding import PartitionSpec as P

QL = 1536
KVL = 512
ROPE = 64
NOPE = 128
VDIM = 128
LONGEST = 2048
LANES = 128
EPSILON = 1e-06
ROPE_BASE = 10000.0
BF16 = jnp.bfloat16
F32 = jnp.float32
MESH = pl.DeviceIdType.MESH


def nt_dot(a, b):
    return lax.dot_general(a, b, (((1,), (1,)), ((), ())), preferred_element_type=F32)


def kernel(
    cfg,
    hid, gain, dpk, qpk, kpk, vpk, q_gain, kv_gain, cosine, sine, first,
    out,
    sc, g_d, g_q, g_k, g_v, p_all, down, kb, kbt, qb, bias, ql, query, s_buf,
    acc, acc_tail, sumsq, total,
    send_sem, recv_sem, p_send, p_recv, z_send, z_recv, x_send, x_recv,
):
    n, n_sub, plane = cfg["n"], cfg["n_sub"], cfg["plane"]
    rows, feat, main = cfg["rows"], cfg["feat"], cfg["main"]
    back, heads = cfg["back"], cfg["heads"]
    share = rows // plane
    z = lax.axis_index("seq")
    me = lax.axis_index("head") * n_sub + lax.axis_index("sub")

    def peer(d):
        other = lax.rem(me + d, plane)
        return {"head": other // n_sub, "sub": lax.rem(other, n_sub)}

    def along(d):
        return {"seq": lax.rem(z + d + n, n)}

    jumps = sorted({1, n - 1, 4, n - 4})
    barrier = pltpu.get_barrier_semaphore()
    for d in jumps:
        pl.semaphore_signal(barrier, inc=1, device_id=along(d), device_id_type=MESH)
    for d in range(1, plane):
        pl.semaphore_signal(barrier, inc=1, device_id=peer(d), device_id_type=MESH)
    pl.semaphore_wait(barrier, len(jumps) + plane - 1)

    dr, qr, kr, vr = dpk.shape[0], qpk.shape[0], kpk.shape[0], vpk.shape[0]
    chunks = []
    pieces = dr // 48 if dr % 48 == 0 else 1
    step = dr // pieces
    for c in range(pieces):
        chunks.append((dpk, g_d, dr, c * step, step))
    chunks.append((kpk, g_k, kr, 0, kr))
    phase_one = list(range(len(chunks)))
    for c in range(3):
        chunks.append((qpk, g_q, qr, c * (qr // 3), qr // 3))
    chunks.append((vpk, g_v, vr, 0, vr))
    phase_two = list(range(len(phase_one), len(chunks)))
    hops = (n - 1 - n // 2, n // 2)
    signs = (1, -1)

    def ring_copy(c, way, step_index, origin, own=False):
        src, held, size, offset, length = chunks[c]
        at = pl.ds(pl.multiple_of(origin * size + offset, 16), length)
        return pltpu.make_async_remote_copy(
            src_ref=src.at[pl.ds(offset, length), :] if own else held.at[at, :],
            dst_ref=held.at[at, :],
            send_sem=send_sem.at[c, way],
            recv_sem=recv_sem.at[c, way, step_index],
            device_id=along(signs[way]),
            device_id_type=MESH,
        )

    def origin_of(way, s):
        return lax.rem(z - signs[way] * s + 2 * n, n)

    def ring_start(which):
        for c in which:
            for way in (0, 1):
                ring_copy(c, way, 0, z, own=True).start()

    def ring_step(which, s, ways, forward):
        for c in which:
            for way in ways:
                origin = origin_of(way, s)
                ring_copy(c, way, s - 1, origin).wait_recv()
                if way in forward:
                    ring_copy(c, way, s - 1, origin).wait_send()
                    ring_copy(c, way, s, origin).start()

    def ring_ways(s):
        ways = [w for w in (0, 1) if s <= hops[w]]
        forward = [w for w in (0, 1) if s < hops[w]]
        return ways, forward

    def ring_finish(which):
        for c in which:
            for way in (0, 1):
                ring_copy(c, way, hops[way] - 1, z).wait_send()

    ring_start(phase_one)

    lane = lax.broadcasted_iota(jnp.int32, (rows, 2 * LANES), 1)
    period = LANES // cfg["gcd"]

    def cut(group, sq):
        base = pl.multiple_of(group * (period * feat), LANES)
        for i in range(period):
            offset = i * feat
            low = offset // LANES * LANES
            shift = offset - low
            width = -(-(shift + feat) // LANES) * LANES
            wide = hid[:, pl.ds(pl.multiple_of(base + low, LANES), width)].astype(F32)
            gains = gain[:, pl.ds(pl.multiple_of(base + low, LANES), width)]
            if shift:
                wide_s = pltpu.roll(wide * gains, width - shift, axis=1)
            else:
                wide_s = wide * gains
            wide_s = wide_s[:, : 2 * LANES]
            kept = jnp.where(lane < feat, wide_s, 0.0)
            sc[group * period + i] = kept.astype(BF16)
        whole = hid[:, pl.ds(base, period * feat)].astype(F32)
        squared = whole * whole
        for t in range(period * feat // LANES):
            sq = sq + squared[:, t * LANES : (t + 1) * LANES]
        return sq

    sumsq[...] = lax.fori_loop(0, n // period, cut, jnp.zeros((rows, LANES), F32))

    acc[...] = jnp.zeros_like(acc)
    acc_tail[...] = jnp.zeros_like(acc_tail)

    def project(origin, own=False):
        lhs = sc[origin]
        if own:
            rhs, tail = dpk[pl.ds(0, feat), :], dpk[pl.ds(feat, 16), :]
        else:
            start = origin * dr
            rhs = g_d[pl.ds(pl.multiple_of(start, 16), feat), :]
            tail = g_d[pl.ds(pl.multiple_of(start + feat, 16), 16), :]
        acc[...] += jnp.dot(lhs[:, :feat], rhs, preferred_element_type=F32)
        acc_tail[...] += nt_dot(lhs, tail)

    project(z, own=True)

    both = min(hops)

    def one_step(s, carry):
        ring_step(phase_one, s, (0, 1), (0, 1))
        project(origin_of(0, s))
        project(origin_of(1, s))
        return carry

    lax.fori_loop(1, both, one_step, 0)
    g_k[pl.ds(pl.multiple_of(z * kr, 16), kr), :] = kpk[...]
    for s in range(both, max(hops) + 1):
        if s == max(hops):
            ring_start(phase_two)
        ways, forward = ring_ways(s)
        ring_step(phase_one, s, ways, forward)
        for way in ways:
            project(origin_of(way, s))
    ring_finish(phase_one)

    def unit(k):
        return kb.at[pl.ds(pl.multiple_of(k * rows + me * share, 16), share), :]

    def p_copy(d):
        return pltpu.make_async_remote_copy(
            src_ref=p_all.at[me], dst_ref=p_all.at[me], send_sem=p_send, recv_sem=p_recv,
            device_id=peer(d), device_id_type=MESH,
        )

    def send_projection():
        mean = jnp.sum(sumsq[...], axis=1, keepdims=True) / (n * feat)
        inverse = lax.rsqrt(mean + EPSILON)
        p_all[me, :, 0:main] = (acc[...] * inverse).astype(BF16)
        p_all[me, :, main : main + LANES] = jnp.zeros((rows, LANES), BF16)
        p_all[me, :, main : main + 16] = (acc_tail[...] * inverse).astype(BF16)
        for d in range(1, plane):
            p_copy(d).start()

    def rope(values):
        w = values.shape[1]
        at = lax.broadcasted_iota(jnp.int32, values.shape, 1)
        swapped = jnp.where(
            lax.rem(at, ROPE) < ROPE // 2,
            pltpu.roll(values, w - ROPE // 2, axis=1),
            pltpu.roll(values, ROPE // 2, axis=1),
        )
        return values * cosine[...] + swapped * sine[...]

    def make_bias():
        query_pos = z * rows + lax.broadcasted_iota(jnp.int32, (rows, rows), 0)
        start = jnp.broadcast_to(first[...], (rows, rows))
        for k in range(back + 1):
            key_pos = (z - k) * rows + lax.broadcasted_iota(jnp.int32, (rows, rows), 1)
            allowed = (key_pos <= query_pos) & (key_pos >= start)
            bias[:, k * rows : (k + 1) * rows] = jnp.where(allowed, 0.0, -jnp.inf)

    def gather_projection():
        several = p_all.at[pl.ds(0, plane - 1)]
        pltpu.make_async_copy(several, several, p_recv).wait()
        down[...] = jnp.zeros_like(down)
        width = main + LANES
        for j in range(plane):
            piece = p_all[j].astype(F32)
            shift = j * cfg["tail"]
            if shift:
                piece = pltpu.roll(piece, shift, axis=1)
            down[:, j * main : j * main + width] += piece
        q = down[:, 0:QL]
        scale = lax.rsqrt(jnp.mean(q * q, axis=1, keepdims=True) + EPSILON)
        ql[...] = (q * scale * q_gain[...]).astype(BF16)
        c = down[:, QL : QL + KVL]
        scale = lax.rsqrt(jnp.mean(c * c, axis=1, keepdims=True) + EPSILON)
        kb[0:rows, 0:KVL] = (c * scale * kv_gain[...]).astype(BF16)
        turned = rope(down[:, QL + KVL : QL + KVL + LANES])
        turned = turned + pltpu.roll(turned, ROPE, axis=1)
        kb[0:rows, KVL : KVL + LANES] = turned.astype(BF16)

    def z_copy(k, jump):
        return pltpu.make_async_remote_copy(
            src_ref=unit(k), dst_ref=unit(k + jump),
            send_sem=z_send.at[k + jump], recv_sem=z_recv.at[k + jump],
            device_id=along(jump), device_id_type=MESH,
        )

    def x_copy(k, d):
        return pltpu.make_async_remote_copy(
            src_ref=unit(k), dst_ref=unit(k), send_sem=x_send.at[k], recv_sem=x_recv.at[k],
            device_id=peer(d), device_id_type=MESH,
        )

    parents = {}
    ticks = {0: [0]}
    for k in range(1, back + 1):
        m, r = k // 4, k % 4
        parents[k] = 1 if r else 4
        ticks.setdefault(m + r, []).append(k)

    def x_bytes(k):
        return kb.at[pl.ds(k * rows, rows - share), :]

    def transpose_slot(k):
        for t in range(kb.shape[1] // LANES):
            tile = kb[k * rows : (k + 1) * rows, t * LANES : (t + 1) * LANES]
            kbt[t * LANES : (t + 1) * LANES, k * rows : (k + 1) * rows] = (
                tile.astype(F32).T.astype(BF16)
            )

    def tick(t):
        arrived = sorted(ticks[t], key=lambda k: k % 4)
        for k in arrived:
            if k:
                z_copy(k - parents[k], parents[k]).wait_recv()
            for jump in (4, 1):
                if k + jump <= back and parents[k + jump] == jump:
                    if jump == 4 and k % 4:
                        continue
                    z_copy(k, jump).start()
        for k in arrived:
            if k:
                for d in range(1, plane):
                    x_copy(k, d).start()

    def settle(t):
        for k in ticks[t]:
            if k:
                pltpu.make_async_copy(x_bytes(k), x_bytes(k), x_recv.at[k]).wait()
            transpose_slot(k)

    last_tick = max(ticks)
    final = max(hops)
    hooks = {0: [send_projection, make_bias]}
    hooks[3] = [gather_projection, functools.partial(tick, 0)]
    when = {0: 3, 1: 5, 2: 7, 3: 9, 4: 11, 5: 13, 6: 15}
    when = {t: min(when.get(t, final), final) for t in range(last_tick + 1)}
    for t in range(1, last_tick + 1):
        hooks.setdefault(when[t], []).append(functools.partial(tick, t))
    late = []
    for t in range(last_tick + 1):
        if when[t] + 2 <= final:
            hooks.setdefault(when[t] + 2, []).append(functools.partial(settle, t))
        else:
            late.append(functools.partial(settle, t))

    for hook in hooks.get(0, []):
        hook()
    g_q[pl.ds(pl.multiple_of(z * qr, 16), qr), :] = qpk[...]
    g_v[pl.ds(pl.multiple_of(z * vr, 16), vr), :] = vpk[...]
    for s in range(1, final + 1):
        ways, forward = ring_ways(s)
        ring_step(phase_two, s, ways, forward)
        for hook in hooks.get(s, []):
            hook()
    for hook in late:
        hook()

    half = heads * NOPE

    def nope_pair(i, carry):
        cols = pl.ds(pl.multiple_of(i * 2 * NOPE, 2 * NOPE), 2 * NOPE)
        two = jnp.dot(ql[...], g_q[:, cols], preferred_element_type=F32).astype(BF16)
        keys = g_k[:, cols]
        for e in range(2):
            absorbed = nt_dot(two[:, e * NOPE : (e + 1) * NOPE], keys[:, e * NOPE : (e + 1) * NOPE])
            at = pl.ds(pl.multiple_of((2 * i + e) * rows, rows), rows)
            qb[at, 0:KVL] = absorbed.astype(BF16)
        cols = pl.ds(pl.multiple_of(half + i * 2 * ROPE, 2 * ROPE), 2 * ROPE)
        two = jnp.dot(ql[...], g_q[:, cols], preferred_element_type=F32).astype(BF16)
        turned = rope(two.astype(F32))
        low = lax.broadcasted_iota(jnp.int32, turned.shape, 1) < ROPE
        for e in range(2):
            kept = jnp.where(low, turned, 0.0) if e == 0 else jnp.where(low, 0.0, turned)
            at = pl.ds(pl.multiple_of((2 * i + e) * rows, rows), rows)
            qb[at, KVL : KVL + LANES] = kept.astype(BF16)
        return carry

    lax.fori_loop(0, heads // 2, nope_pair, 0)

    scale = (NOPE + ROPE) ** (-0.5)
    keys_total = (back + 1) * rows

    def one_head(h, carry):
        at = pl.ds(pl.multiple_of(h * rows, rows), rows)
        q = qb[at, :]
        top = jnp.full((rows, LANES), -jnp.inf, F32)
        for first_key in range(0, keys_total, 512):
            size = min(512, keys_total - first_key)
            s = jnp.dot(q, kbt[:, first_key : first_key + size], preferred_element_type=F32)
            s = s * scale + bias[:, first_key : first_key + size]
            s_buf[:, first_key : first_key + size] = s
            for t in range(size // LANES):
                top = jnp.maximum(top, s[:, t * LANES : (t + 1) * LANES])
        top = jnp.max(top, axis=1, keepdims=True)
        summed = jnp.zeros((rows, LANES), F32)
        mixed = jnp.zeros((rows, KVL), F32)
        for first_key in range(0, keys_total, 512):
            size = min(512, keys_total - first_key)
            p = jnp.exp(s_buf[:, first_key : first_key + size] - top)
            for t in range(size // LANES):
                summed = summed + p[:, t * LANES : (t + 1) * LANES]
            mixed = mixed + jnp.dot(
                p.astype(BF16), kb[first_key : first_key + size, 0:KVL],
                preferred_element_type=F32,
            )
        sums = jnp.sum(summed, axis=1, keepdims=True)
        mixed = (mixed / sums).astype(BF16)
        cols = pl.ds(pl.multiple_of(h * VDIM, VDIM), VDIM)
        out[:, cols] = jnp.dot(mixed, g_v[:, cols], preferred_element_type=F32).astype(BF16)
        return carry

    lax.fori_loop(0, heads, one_head, 0)

    ring_finish(phase_two)
    several = p_all.at[pl.ds(0, plane - 1)]
    pltpu.make_async_copy(several, several, p_send).wait()
    for k in range(1, back + 1):
        z_copy(k - parents[k], parents[k]).wait_send()
        pltpu.make_async_copy(x_bytes(k), x_bytes(k), x_send.at[k]).wait()


def local(mesh, hidden, segment_ids, attn_gain, down_weight, q_gain, kv_gain, q_up, key_up, value_up):
    n, n_head, n_sub = mesh.shape["seq"], mesh.shape["head"], mesh.shape["sub"]
    plane = n_head * n_sub
    rows, width = hidden.shape
    feat, cols = down_weight.shape
    main = cols // LANES * LANES
    tail = cols - main
    heads = q_up.shape[1] // (NOPE + ROPE)
    back = -(-(LONGEST - 1) // rows)

    z = lax.axis_index("seq")
    positions = z * rows + jnp.arange(rows, dtype=jnp.int32)
    half = ROPE // 2
    frequency = ROPE_BASE ** (-jnp.arange(half, dtype=F32) / half)
    angles = positions.astype(F32)[:, None] * frequency[None, :]
    cosine, sine = jnp.cos(angles), jnp.sin(angles)
    cosine = jnp.concatenate([cosine] * 4, axis=1)
    sine = jnp.concatenate([-sine, sine, -sine, sine], axis=1)
    own = lax.dynamic_slice_in_dim(segment_ids, z * rows, rows, 0)
    first = jnp.sum((segment_ids[None, :] < own[:, None]).astype(jnp.int32), axis=1, keepdims=True)

    tails = jnp.pad(down_weight[:, main:].T, ((0, 16 - tail), (0, main - feat)))
    dpk = jnp.concatenate([down_weight[:, :main], tails], axis=0)
    by_head = q_up.reshape(q_up.shape[0], heads, NOPE + ROPE)
    qpk = jnp.concatenate(
        [by_head[:, :, :NOPE].reshape(-1, heads * NOPE), by_head[:, :, NOPE:].reshape(-1, heads * ROPE)],
        axis=1,
    )
    kpk = key_up.T
    cfg = dict(
        n=n, n_sub=n_sub, plane=plane, rows=rows, feat=feat, main=main, tail=tail,
        back=back, heads=heads, gcd=math.gcd(feat, LANES),
    )
    window = (back + 1) * rows
    n_chunks = (dpk.shape[0] // 48 if dpk.shape[0] % 48 == 0 else 1) + 5
    vmem = pltpu.VMEM
    scratch = [
        vmem((n, rows, 2 * LANES), BF16),
        vmem((n * dpk.shape[0], main), BF16),
        vmem((QL, qpk.shape[1]), BF16),
        vmem((KVL, kpk.shape[1]), BF16),
        vmem((KVL, value_up.shape[1]), BF16),
        vmem((plane, rows, main + LANES), BF16),
        vmem((rows, plane * main + LANES), F32),
        vmem((window, KVL + LANES), BF16),
        vmem((KVL + LANES, window), BF16),
        vmem((heads * rows, KVL + LANES), BF16),
        vmem((rows, window), F32),
        vmem((rows, QL), BF16),
        vmem((16, LANES), BF16),
        vmem((rows, window), F32),
        vmem((rows, main), F32),
        vmem((rows, 16), F32),
        vmem((rows, LANES), F32),
        vmem((8, LANES), F32),
        pltpu.SemaphoreType.DMA((n_chunks, 2)),
        pltpu.SemaphoreType.DMA((n_chunks, 2, n // 2)),
        pltpu.SemaphoreType.DMA,
        pltpu.SemaphoreType.DMA,
        pltpu.SemaphoreType.DMA((back + 1,)),
        pltpu.SemaphoreType.DMA((back + 1,)),
        pltpu.SemaphoreType.DMA((back + 1,)),
        pltpu.SemaphoreType.DMA((back + 1,)),
    ]
    return pl.pallas_call(
        functools.partial(kernel, cfg),
        out_shape=jax.ShapeDtypeStruct((rows, heads * VDIM), BF16),
        in_specs=[pl.BlockSpec(memory_space=pltpu.VMEM)] * 11,
        out_specs=pl.BlockSpec(memory_space=pltpu.VMEM),
        scratch_shapes=scratch,
        compiler_params=pltpu.CompilerParams(
            collective_id=0, has_side_effects=True, vmem_limit_bytes=60 * 1024 * 1024
        ),
    )(
        hidden, attn_gain[None, :], dpk, qpk, kpk, value_up, q_gain[None, :], kv_gain[None, :],
        cosine, sine, first,
    )


def solution(mesh):
    placed = (
        P(("groups", "seq"), None),
        P("groups"),
        P(),
        P("seq", ("head", "sub")),
        P(),
        P(),
        P("seq", ("head", "sub")),
        P(("head", "sub"), "seq"),
        P("seq", ("head", "sub")),
    )
    return jax.shard_map(
        functools.partial(local, mesh),
        mesh=mesh,
        in_specs=placed,
        out_specs=P(("groups", "seq"), ("head", "sub")),
        check_vma=False,
    )
```

```python
import functools
import math

import jax
import jax.numpy as jnp
import numpy as np
from jax import lax
from jax.experimental import pallas as pl
from jax.experimental.pallas import tpu as pltpu
from jax.sharding import PartitionSpec as P

QL = 1536
KVL = 512
ROPE = 64
NOPE = 128
VDIM = 128
LONGEST = 2048
LANES = 128
EPSILON = 1e-06
ROPE_BASE = 10000.0
BF16 = jnp.bfloat16
F32 = jnp.float32
MESH = pl.DeviceIdType.MESH


def nt_dot(a, b):
    return lax.dot_general(a, b, (((1,), (1,)), ((), ())), preferred_element_type=F32)


def kernel(
    cfg,
    hid, gain, segs, dw, qw, kw, vw, q_gain, kv_gain, freq,
    out,
    sc, g_d, g_t, g_q, g_kv, p_all, p_key, down, kd, mine, kb, kbt, qb, bias, ql, s_buf,
    acc, acc_tail, sumsq, cosine, sine, tails, turn,
    send_sem, recv_sem, y_send, y_recv, p_sem, k_sem, z_send, z_recv, x_send, x_recv,
):
    n, n_head, n_sub, plane = cfg["n"], cfg["n_head"], cfg["n_sub"], cfg["plane"]
    rows, feat, main, tail = cfg["rows"], cfg["feat"], cfg["main"], cfg["tail"]
    back, heads = cfg["back"], cfg["heads"]
    share = rows // plane
    wide = main + LANES
    z, head, sub = lax.axis_index("seq"), lax.axis_index("head"), lax.axis_index("sub")
    me = head * n_sub + sub
    group = lax.axis_index("groups")
    parity = lax.rem(group, 2)
    pair = {"groups": group + 1 - 2 * parity}

    def peer(d):
        other = lax.rem(me + d, plane)
        return {"head": other // n_sub, "sub": lax.rem(other, n_sub)}

    def along(d):
        return {"seq": lax.rem(z + d + n, n)}

    sibling = {"sub": 1 - sub}

    def column(d):
        return {"head": lax.rem(head + d, n_head)}

    jumps = sorted({1, n - 1, 4, n - 4})
    barrier = pltpu.get_barrier_semaphore()
    for d in jumps:
        pl.semaphore_signal(barrier, inc=1, device_id=along(d), device_id_type=MESH)
    for d in range(1, plane):
        pl.semaphore_signal(barrier, inc=1, device_id=peer(d), device_id_type=MESH)
    pl.semaphore_signal(barrier, inc=1, device_id=pair, device_id_type=MESH)
    pl.semaphore_wait(barrier, len(jumps) + plane)

    dr, qr, kr = feat, qw.shape[0], kw.shape[0]
    common, half_rows = cfg["d_common"], (feat - cfg["d_common"]) // 2
    q_third = qr // 3

    def rows_of(src, held, size, offset, length, lanes=None):
        def own(par):
            at = pl.ds(offset(par), length)
            return src.at[at, pl.ds(0, lanes)] if lanes else src.at[at, :]

        def there(o, par):
            return held.at[pl.ds(pl.multiple_of(o * size + offset(par), 16), length), :]

        return own, there

    def fixed(offset):
        return lambda par: offset

    def kv_there(o, par):
        return g_kv.at[pl.ds(pl.multiple_of(par * KVL + o * kr, 16), kr), :]

    chunks = [
        rows_of(dw, g_d, dr, lambda par: pl.multiple_of(common + par * half_rows, 16), half_rows, main),
        rows_of(dw, g_d, dr, fixed(0), common // 2, main),
        rows_of(dw, g_d, dr, fixed(common // 2), common // 2, main),
        rows_of(tails, g_t, 16, fixed(0), 16),
        (None, kv_there),
        rows_of(qw, g_q, qr, lambda par: pl.multiple_of(q_third * (1 + par), 16), q_third),
        rows_of(qw, g_q, qr, fixed(0), q_third),
    ]
    D_SHARED, TAIL, KV, Q_SHARED = 0, 3, 4, 5
    shared = {D_SHARED: 0, KV: 1, Q_SHARED: 2}
    phase_one, phase_two = [0, 1, 2, 3, 4], [5, 6]
    hops = (n - 1 - n // 2, n // 2)
    signs = (1, -1)

    def ring_copy(c, way, step_index, origin, src=None):
        there = chunks[c][1](origin, parity)
        return pltpu.make_async_remote_copy(
            src_ref=there if src is None else src,
            dst_ref=there,
            send_sem=send_sem.at[c, way],
            recv_sem=recv_sem.at[c, way, step_index],
            device_id=along(signs[way]),
            device_id_type=MESH,
        )

    def pair_copy(c, way, step_index, origin, par):
        there = chunks[c][1](origin, par)
        return pltpu.make_async_remote_copy(
            src_ref=there,
            dst_ref=there,
            send_sem=y_send.at[shared[c], way],
            recv_sem=y_recv.at[shared[c], way, step_index],
            device_id=pair,
            device_id_type=MESH,
        )

    def origin_of(way, s):
        return lax.rem(z - signs[way] * s + 2 * n, n)

    def ring_start(which):
        for c in which:
            for way in (0, 1):
                if c == KV:
                    for par, src in enumerate((kw, vw)):
                        @pl.when(parity == par)
                        def _():
                            ring_copy(c, way, 0, z, src=src).start()
                else:
                    ring_copy(c, way, 0, z, src=chunks[c][0](parity)).start()

    def ring_step(which, s, first=False):
        static = isinstance(s, int)
        for c in which:
            for way in (0, 1):
                if static and s > hops[way]:
                    continue
                origin = origin_of(way, s)
                copy = ring_copy(c, way, s - 1, origin)
                copy.wait_recv()
                if not static or s < hops[way]:
                    copy.wait_send()
                    ring_copy(c, way, s, origin).start()
                if c in shared:
                    if not first:
                        pair_copy(c, way, s - 1, origin, parity).wait_send()
                    pair_copy(c, way, s - 1, origin, parity).start()

    def pair_wait(c, s):
        for way in (0, 1):
            if not isinstance(s, int) or s <= hops[way]:
                pair_copy(c, way, s - 1, origin_of(way, s), 1 - parity).wait_recv()

    def ring_finish(which):
        for c in which:
            for way in (0, 1):
                ring_copy(c, way, hops[way] - 1, z).wait_send()
                if c in shared:
                    pair_copy(c, way, hops[way] - 1, z, parity).wait_send()

    ring_start([c for c in phase_one if c != TAIL])

    turn[...] = jnp.zeros_like(turn)
    turn[0:feat, 0:tail] = dw[:, main : main + tail].astype(F32)
    for t in range(main // LANES):
        flat = turn[t * LANES : (t + 1) * LANES, :].T
        tails[:, t * LANES : (t + 1) * LANES] = flat[0:16, :].astype(BF16)

    lane = lax.broadcasted_iota(jnp.int32, (rows, 2 * LANES), 1)
    period = LANES // math.gcd(feat, LANES)
    per_group = period * feat // LANES

    def cut(g, sq):
        tiles = []
        for t in range(per_group):
            at = pl.ds(pl.multiple_of((g * per_group + t) * LANES, LANES), LANES)
            tile = hid[:, at].astype(F32)
            sq = sq + tile * tile
            tiles.append(tile * gain[pl.ds(g * per_group + t, 1), :])
        for i in range(period):
            low, shift = i * feat // LANES, i * feat % LANES
            high = -(-(i * feat + feat) // LANES)
            part = jnp.concatenate(tiles[low:high], axis=1)
            if shift:
                part = pltpu.roll(part, part.shape[1] - shift, axis=1)
            kept = jnp.where(lane < feat, part[:, : 2 * LANES], 0.0)
            sc[g * period + i] = kept.astype(BF16)
        return sq

    sumsq[...] = lax.fori_loop(0, n // period, cut, jnp.zeros((rows, LANES), F32))
    ring_start([TAIL])

    acc[...] = jnp.zeros_like(acc)
    acc_tail[...] = jnp.zeros_like(acc_tail)

    def project(origin, own=False):
        lhs = sc[origin]
        if own:
            rhs, last = dw[:, 0:main], tails[...]
        else:
            rhs = g_d[pl.ds(pl.multiple_of(origin * feat, 16), feat), :]
            last = g_t[pl.ds(pl.multiple_of(origin * 16, 16), 16), :]
        acc[...] += jnp.dot(lhs[:, :feat], rhs, preferred_element_type=F32)
        acc_tail[...] += nt_dot(lhs, last)

    def project_step(s):
        pair_wait(D_SHARED, s)
        for way in (0, 1):
            if not isinstance(s, int) or s <= hops[way]:
                project(origin_of(way, s))

    def unit(k):
        return kb.at[pl.ds(pl.multiple_of(k * rows + me * share, 16), share), :]

    def peer_index(d):
        return lax.rem(head + d, n_head) * n_sub + sub

    P_COL, P_SIB, P_COL_OUT, P_SIB_OUT = 0, 1, 2, 3

    def p_copy(j, device, out_sem, in_sem):
        return pltpu.make_async_remote_copy(
            src_ref=p_all.at[j], dst_ref=p_all.at[j],
            send_sem=p_sem.at[out_sem], recv_sem=p_sem.at[in_sem],
            device_id=device, device_id_type=MESH,
        )

    def k_copy(d):
        other = lax.rem(me + d, plane)
        return pltpu.make_async_remote_copy(
            src_ref=p_all.at[me, pl.ds(pl.multiple_of(other * share, 16), share), :],
            dst_ref=p_key.at[me],
            send_sem=k_sem.at[0], recv_sem=k_sem.at[1],
            device_id=peer(d), device_id_type=MESH,
        )

    def wait_bytes(ref, sem):
        pltpu.make_async_copy(ref, ref, sem).wait()

    def send_projection():
        mean = jnp.sum(sumsq[...], axis=1, keepdims=True) / (n * feat)
        inverse = lax.rsqrt(mean + EPSILON)
        p_all[me, :, 0:main] = (acc[...] * inverse).astype(BF16)
        p_all[me, :, main:wide] = jnp.zeros((rows, LANES), BF16)
        p_all[me, :, main : main + 16] = (acc_tail[...] * inverse).astype(BF16)
        for d in range(1, plane):
            k_copy(d).start()
        for d in range(1, n_head):
            p_copy(me, column(d), P_COL_OUT, P_COL).start()
        p_copy(me, sibling, P_SIB_OUT, P_SIB).start()
        p_key[me] = p_all[me, pl.ds(pl.multiple_of(me * share, 16), share), :]

    def relay_projection():
        wait_bytes(p_all.at[pl.ds(0, n_head - 1)], p_sem.at[P_COL])
        for d in range(1, n_head):
            p_copy(peer_index(d), sibling, P_SIB_OUT, P_SIB).start()

    def rope(values, cos, sin):
        w = values.shape[1]
        at = lax.broadcasted_iota(jnp.int32, values.shape, 1)
        swapped = jnp.where(
            lax.rem(at, ROPE) < ROPE // 2,
            pltpu.roll(values, w - ROPE // 2, axis=1),
            pltpu.roll(values, ROPE // 2, axis=1),
        )
        return values * cos + swapped * sin

    def normed(values, gains):
        scale = lax.rsqrt(jnp.mean(values * values, axis=1, keepdims=True) + EPSILON)
        parts = []
        for t in range(values.shape[1] // LANES):
            part = values[:, t * LANES : (t + 1) * LANES]
            parts.append((part * scale * gains[t : t + 1, :]).astype(BF16))
        return parts

    def write_keys(target, columns, cos, sin):
        count = columns.shape[0]
        for t, part in enumerate(normed(columns[:, 0:KVL], kv_gain)):
            target[0:count, t * LANES : (t + 1) * LANES] = part
        turned = rope(columns[:, KVL : KVL + LANES], cos, sin)
        turned = turned + pltpu.roll(turned, ROPE, axis=1)
        target[0:count, KVL : KVL + LANES] = turned.astype(BF16)

    first_key = QL // (main + tail)
    key_lane = QL - first_key * main

    def key_share():
        wait_bytes(p_key.at[pl.ds(0, plane - 1)], k_sem.at[1])
        kd[...] = jnp.zeros_like(kd)
        for j in range(first_key, plane):
            piece = pltpu.roll(p_key[j].astype(F32), j * tail, axis=1)
            low = (j - first_key) * main
            kd[:, low : low + wide] += piece
        at = pl.ds(pl.multiple_of(me * share, 16), share)
        write_keys(mine, kd[:, key_lane : key_lane + KVL + LANES], cosine[at, :], sine[at, :])

    def tables():
        position = z * rows + lax.broadcasted_iota(jnp.int32, (rows, LANES), 0)
        angles = position.astype(F32) * freq[...]
        at = lax.broadcasted_iota(jnp.int32, (rows, LANES), 1)
        cosine[...] = jnp.cos(angles)
        sine[...] = jnp.where(lax.rem(at, ROPE) < ROPE // 2, -1.0, 1.0) * jnp.sin(angles)

    def make_bias():
        query_pos = z * rows + lax.broadcasted_iota(jnp.int32, (rows, rows), 0)
        own = jnp.broadcast_to(segs[pl.ds(z, 1), :], (rows, rows)).T
        for k in range(back + 1):
            key_pos = (z - k) * rows + lax.broadcasted_iota(jnp.int32, (rows, rows), 1)
            seg = segs[pl.ds(lax.rem(z - k + 2 * n, n), 1), :]
            allowed = (key_pos <= query_pos) & (key_pos >= 0) & (seg == own)
            bias[:, k * rows : (k + 1) * rows] = jnp.where(allowed, 0.0, -jnp.inf)

    def gather_projection():
        wait_bytes(p_all.at[pl.ds(0, n_head)], p_sem.at[P_SIB])
        down[...] = jnp.zeros_like(down)
        for j in range(plane):
            piece = p_all[j].astype(F32)
            if j:
                piece = pltpu.roll(piece, j * tail, axis=1)
            down[:, j * main : j * main + wide] += piece
        for t, part in enumerate(normed(down[:, 0:QL], q_gain)):
            ql[:, t * LANES : (t + 1) * LANES] = part
        write_keys(kb, down[:, QL : QL + KVL + LANES], cosine[...], sine[...])

    def z_copy(k, jump):
        return pltpu.make_async_remote_copy(
            src_ref=unit(k) if k else mine, dst_ref=unit(k + jump),
            send_sem=z_send.at[k + jump], recv_sem=z_recv.at[k + jump],
            device_id=along(jump), device_id_type=MESH,
        )

    def x_copy(k, j, device, out_sem, in_sem):
        ref = kb.at[pl.ds(pl.multiple_of(k * rows + j * share, 16), share), :]
        return pltpu.make_async_remote_copy(
            src_ref=ref, dst_ref=ref, send_sem=x_send.at[out_sem, k], recv_sem=x_recv.at[in_sem, k],
            device_id=device, device_id_type=MESH,
        )

    parents, ticks = {}, {0: [0]}
    for k in range(1, back + 1):
        parents[k] = 1 if k % 4 else 4
        ticks.setdefault(k // 4 + k % 4, []).append(k)

    def x_bytes(k, units):
        return kb.at[pl.ds(k * rows, units * share), :]

    def transpose_slot(k):
        for t in range(kb.shape[1] // LANES):
            tile = kb[k * rows : (k + 1) * rows, t * LANES : (t + 1) * LANES]
            kbt[t * LANES : (t + 1) * LANES, k * rows : (k + 1) * rows] = (
                tile.astype(F32).T.astype(BF16)
            )

    def tick(t):
        arrived = sorted(ticks[t], key=lambda k: k % 4)
        for k in arrived:
            if k:
                z_copy(k - parents[k], parents[k]).wait_recv()
            for jump in (4, 1):
                if k + jump <= back and parents[k + jump] == jump:
                    if jump == 4 and k % 4:
                        continue
                    z_copy(k, jump).start()
        for k in arrived:
            if k:
                for d in range(1, n_head):
                    x_copy(k, me, column(d), 0, 0).start()
                x_copy(k, me, sibling, 1, 1).start()

    def relay(t):
        for k in ticks[t]:
            if k:
                wait_bytes(x_bytes(k, n_head - 1), x_recv.at[0, k])
                for d in range(1, n_head):
                    x_copy(k, peer_index(d), sibling, 1, 1).start()

    def settle(t):
        for k in ticks[t]:
            if k:
                wait_bytes(x_bytes(k, n_head), x_recv.at[1, k])
            transpose_slot(k)

    project(z, own=True)
    tables()
    q_start = min(cfg["q_start"], max(hops))
    last_d, final = max(hops), q_start + max(hops)
    ring_step(phase_one, 1, first=True)

    def one_step(s, carry):
        ring_step(phase_one, s)
        project_step(s - 1)
        return carry

    lax.fori_loop(2, min(q_start, min(hops)), one_step, 0)
    for par, src in enumerate((kw, vw)):
        g_kv[pl.ds(pl.multiple_of(par * KVL + z * kr, 16), kr), :] = src[...]
    g_q[pl.ds(pl.multiple_of(z * qr, 16), qr), :] = qw[...]

    hooks = {}

    def at_tick(when, what, *args):
        hooks.setdefault(min(when, final), []).append(functools.partial(what, *args))

    base = last_d
    at_tick(base, send_projection)
    at_tick(base, make_bias)
    at_tick(base + 1, key_share)
    at_tick(base + 1, tick, 0)
    at_tick(base + 2, relay_projection)
    for t, when in enumerate(cfg["when"], start=1):
        at_tick(base + when, tick, t)
    for t, when in enumerate(cfg["relay"], start=1):
        at_tick(base + when, relay, t)
    at_tick(base + 5, gather_projection)
    at_tick(base + 6, settle, 0)
    for t, when in enumerate(cfg["settle"], start=1):
        at_tick(base + when, settle, t)

    for step in range(min(q_start, min(hops)), final + 1):
        if step <= last_d:
            ring_step(phase_one, step)
        if step == q_start:
            ring_start(phase_two)
        elif step > q_start:
            ring_step(phase_two, step - q_start, first=step == q_start + 1)
        if step <= last_d:
            project_step(step - 1)
        if step == last_d:
            project_step(step)
        for hook in hooks.get(step, []):
            hook()

    def collect(s, carry):
        pair_wait(KV, s)
        pair_wait(Q_SHARED, s)
        return carry

    lax.fori_loop(1, min(hops) + 1, collect, 0)
    pair_wait(KV, max(hops))
    pair_wait(Q_SHARED, max(hops))

    low = lax.broadcasted_iota(jnp.int32, (rows, LANES), 1) < ROPE

    def query_pair(i, carry):
        width = 2 * (NOPE + ROPE)
        cols = pl.ds(pl.multiple_of(i * width, width), width)
        two = jnp.dot(ql[...], g_q[:, cols], preferred_element_type=F32).astype(BF16).astype(F32)
        one, middle, end = two[:, 0:LANES], two[:, LANES : 2 * LANES], two[:, 2 * LANES :]
        other = jnp.where(low, pltpu.roll(middle, ROPE, axis=1), pltpu.roll(end, ROPE, axis=1))
        turned = rope(jnp.where(low, middle, end), cosine[...], sine[...])
        for e, nope in enumerate((one, other)):
            lanes = pl.ds(pl.multiple_of((2 * i + e) * NOPE, NOPE), NOPE)
            absorbed = nt_dot(nope.astype(BF16), g_kv[0:KVL, lanes])
            at = pl.ds(pl.multiple_of((2 * i + e) * rows, rows), rows)
            qb[at, 0:KVL] = absorbed.astype(BF16)
            kept = jnp.where(low, turned, 0.0) if e == 0 else jnp.where(low, 0.0, turned)
            qb[at, KVL : KVL + LANES] = kept.astype(BF16)
        return carry

    lax.fori_loop(0, heads // 2, query_pair, 0)

    scale = (NOPE + ROPE) ** (-0.5)
    keys_total = (back + 1) * rows

    def one_head(h, carry):
        at = pl.ds(pl.multiple_of(h * rows, rows), rows)
        q = qb[at, :]
        top = jnp.full((rows, LANES), -jnp.inf, F32)
        for first_key in range(0, keys_total, 512):
            size = min(512, keys_total - first_key)
            s = jnp.dot(q, kbt[:, first_key : first_key + size], preferred_element_type=F32)
            s = s * scale + bias[:, first_key : first_key + size]
            s_buf[:, first_key : first_key + size] = s
            for t in range(size // LANES):
                top = jnp.maximum(top, s[:, t * LANES : (t + 1) * LANES])
        top = jnp.max(top, axis=1, keepdims=True)
        summed = jnp.zeros((rows, LANES), F32)
        mixed = jnp.zeros((rows, KVL), F32)
        for first_key in range(0, keys_total, 512):
            size = min(512, keys_total - first_key)
            p = jnp.exp(s_buf[:, first_key : first_key + size] - top)
            for t in range(size // LANES):
                summed = summed + p[:, t * LANES : (t + 1) * LANES]
            mixed = mixed + jnp.dot(
                p.astype(BF16), kb[first_key : first_key + size, 0:KVL],
                preferred_element_type=F32,
            )
        sums = jnp.sum(summed, axis=1, keepdims=True)
        mixed = (mixed / sums).astype(BF16)
        cols = pl.ds(pl.multiple_of(h * VDIM, VDIM), VDIM)
        out[:, cols] = jnp.dot(mixed, g_kv[KVL : 2 * KVL, cols], preferred_element_type=F32).astype(BF16)
        return carry

    lax.fori_loop(0, heads, one_head, 0)

    ring_finish(phase_one)
    ring_finish(phase_two)
    wait_bytes(p_all.at[pl.ds(0, n_head - 1)], p_sem.at[P_COL_OUT])
    wait_bytes(p_all.at[pl.ds(0, n_head)], p_sem.at[P_SIB_OUT])
    wait_bytes(p_key.at[pl.ds(0, plane - 1)], k_sem.at[0])
    for k in range(1, back + 1):
        z_copy(k - parents[k], parents[k]).wait_send()
        wait_bytes(x_bytes(k, n_head - 1), x_send.at[0, k])
        wait_bytes(x_bytes(k, n_head), x_send.at[1, k])


def local(mesh, hidden, segment_ids, attn_gain, down_weight, q_gain, kv_gain, q_up, key_up, value_up):
    n, n_head, n_sub = mesh.shape["seq"], mesh.shape["head"], mesh.shape["sub"]
    plane = n_head * n_sub
    rows = hidden.shape[0]
    feat, cols = down_weight.shape
    main = cols // LANES * LANES
    heads = q_up.shape[1] // (NOPE + ROPE)
    back = -(-(LONGEST - 1) // rows)
    half = ROPE // 2
    exponent = -np.arange(half, dtype=np.float32) / np.float32(half)
    freq = np.tile(np.float32(ROPE_BASE) ** exponent, LANES // half)[None, :]
    cfg = dict(
        n=n, n_head=n_head, n_sub=n_sub, plane=plane, rows=rows, feat=feat, main=main,
        tail=cols - main, back=back, heads=heads, d_common=96, q_start=11,
        when=(3, 5, 7, 9, 10, 11), relay=(4, 6, 8, 10, 11, 12), settle=(5, 7, 9, 11, 12, 13),
    )
    window = (back + 1) * rows
    n_chunks, reach = 7, n // 2
    vmem, dma = pltpu.VMEM, pltpu.SemaphoreType.DMA
    scratch = [
        vmem((n, rows, 2 * LANES), BF16),
        vmem((n * feat, main), BF16),
        vmem((n * 16, main), BF16),
        vmem(q_up.shape[:0] + (QL, q_up.shape[1]), BF16),
        vmem((2 * KVL, value_up.shape[1]), BF16),
        vmem((plane, rows, main + LANES), BF16),
        vmem((plane, rows // plane, main + LANES), BF16),
        vmem((rows, plane * main + LANES), F32),
        vmem((rows // plane, (plane - QL // cols) * main + LANES), F32),
        vmem((rows // plane, KVL + LANES), BF16),
        vmem((window, KVL + LANES), BF16),
        vmem((KVL + LANES, window), BF16),
        vmem((heads * rows, KVL + LANES), BF16),
        vmem((rows, window), F32),
        vmem((rows, QL), BF16),
        vmem((rows, window), F32),
        vmem((rows, main), F32),
        vmem((rows, 16), F32),
        vmem((rows, LANES), F32),
        vmem((rows, LANES), F32),
        vmem((rows, LANES), F32),
        vmem((16, main), BF16),
        vmem((main, LANES), F32),
        dma((n_chunks, 2)),
        dma((n_chunks, 2, reach)),
        dma((3, 2)),
        dma((3, 2, reach)),
        dma((4,)),
        dma((2,)),
        dma((back + 1,)),
        dma((back + 1,)),
        dma((2, back + 1)),
        dma((2, back + 1)),
    ]
    return pl.pallas_call(
        functools.partial(kernel, cfg),
        out_shape=jax.ShapeDtypeStruct((rows, heads * VDIM), BF16),
        in_specs=[pl.BlockSpec(memory_space=pltpu.VMEM)] * 10,
        out_specs=pl.BlockSpec(memory_space=pltpu.VMEM),
        scratch_shapes=scratch,
        compiler_params=pltpu.CompilerParams(
            collective_id=0, has_side_effects=True, vmem_limit_bytes=60 * 1024 * 1024
        ),
    )(
        hidden, attn_gain.reshape(-1, LANES), segment_ids.reshape(n, rows), down_weight, q_up, key_up.T,
        value_up, q_gain.reshape(-1, LANES), kv_gain.reshape(-1, LANES), jnp.asarray(freq),
    )


def solution(mesh):
    placed = (
        P(("groups", "seq"), None),
        P("groups"),
        P(),
        P("seq", ("head", "sub")),
        P(),
        P(),
        P("seq", ("head", "sub")),
        P(("head", "sub"), "seq"),
        P("seq", ("head", "sub")),
    )
    return jax.shard_map(
        functools.partial(local, mesh),
        mesh=mesh,
        in_specs=placed,
        out_specs=P(("groups", "seq"), ("head", "sub")),
        check_vma=False,
    )
```
